32 devices in a mesh: subj: 16 (over z, y, x), vox: 2 (over core).
Axes of the slice: x: 2, y: 2, z: 4, core: 2. Of those that a mesh axis runs over, the one named last changes fastest.
Arguments:
- bold_series: float32 [16, 300, 16384], P('subj', None, 'vox')
- seed_index: int32 [256], replicated, may hold values from 0 to 16383
Outputs:
- group_z: float32 [16384, 256], P(('vox', 'subj'))
The draws below stay inside these ranges and needn't reach their ends.
All inputs are finite; a program needn't handle non-finite values.
Results may differ from the reference program's by a relative error of at most 0.00031.
Values may be sent and summed in bfloat16 or wider, within the bound.
No kernel may reach another device: no remote copies, remote signals or barrier semaphores. Data moves between devices by JAX's collectives and lax.ppermute only.
A program may use at most 64 MiB of HBM per device.

```python
import math
import jax
import jax.numpy as jnp
from jax import lax

TIMEPOINTS = 300
SEEDS = 256
SUBJ = 16
VOXELS = 16384


def draw_bold_series(key, part):
    factors = 4
    subkeys = jax.random.split(key, 6)
    hidden_factors = jax.random.normal(subkeys[0], (SUBJ, factors, TIMEPOINTS), jnp.float32)
    common_component = jax.random.normal(subkeys[1], (factors, VOXELS), jnp.float32) * (0.8 / math.sqrt(factors))
    subject_specific = jax.random.normal(subkeys[2], (SUBJ, factors, VOXELS), jnp.float32) * (0.6 / math.sqrt(factors))
    signal_component = jnp.einsum('oju,ojf->ouf', hidden_factors, common_component[None] + subject_specific)
    noise_part = jax.random.normal(subkeys[3], (SUBJ, TIMEPOINTS, VOXELS), jnp.float32)
    scale_factors = jnp.exp(jax.random.uniform(subkeys[4], (SUBJ, 1, VOXELS), jnp.float32, 0.0, math.log(10.0)))
    offsets = jax.random.uniform(subkeys[5], (SUBJ, 1, VOXELS), jnp.float32, -5.0, 5.0)
    return offsets + scale_factors * (signal_component + noise_part)


def place_ends(drawn, rng, smallest, largest):
    longest = drawn.shape.index(max(drawn.shape))
    spots = []
    for shift in (0, 1):
        where = [jax.random.randint(jax.random.fold_in(rng, axis), (), 0, length) for axis, length in enumerate(drawn.shape)]
        where[longest] = (where[longest] + shift) % drawn.shape[longest]
        spots.append(tuple(where))
    return drawn.at[spots[0]].set(smallest).at[spots[1]].set(largest)


def setup_inputs(seed: int = 0) -> dict:
    arg_keys = jax.random.split(jax.random.key(seed), 3)
    return {
        "bold_series": draw_bold_series(jax.random.fold_in(arg_keys[2], 71), 0),
        "seed_index": place_ends(jax.random.randint(arg_keys[1], (SEEDS,), 0, VOXELS), jax.random.fold_in(arg_keys[1], 1), 0, VOXELS - 1).astype(jnp.int32),
    }


clip_limit = 0.99
epsilon = 1e-05

def normalize(series):
    demean_series = series - lax.optimization_barrier(jnp.mean(series, axis=0, keepdims=True))
    spread = lax.optimization_barrier(jnp.mean(demean_series * demean_series, axis=0, keepdims=True))
    return (demean_series * lax.rsqrt(spread + epsilon)).astype(jnp.bfloat16)

def arctanh_transform(cross_product, length):
    clipped = jnp.clip(cross_product * (1.0 / length), -clip_limit, clip_limit)
    return 0.5 * jnp.log((1.0 + clipped) / (1.0 - clipped))

def reference(bold_series, seed_index):
    length = bold_series.shape[1]

    def accumulate(summed, series):
        normed = normalize(series)
        seed_panel = jnp.take(normed, seed_index.astype(jnp.int32), axis=1)
        cross_product = lax.dot_general(normed, seed_panel, (((0,), (0,)), ((), ())), preferred_element_type=jnp.float32)
        return (summed + arctanh_transform(cross_product, length), None)
    start_sum = jnp.zeros((bold_series.shape[2], seed_index.shape[0]), jnp.float32)
    summed, unused = lax.scan(accumulate, start_sum, bold_series)
    return summed * (1.0 / SUBJ)
```

```python
import math

import jax
import jax.numpy as jnp
import numpy as np
from jax import lax
from jax.experimental import pallas as pl
from jax.experimental.pallas import tpu as pltpu
from jax.sharding import PartitionSpec as P

clip_limit = 0.99
epsilon = 1e-05
colours = 4
floor_z = 2.0**-11
levels = 32700.0

params = pltpu.CompilerParams(
    dimension_semantics=("arbitrary",), vmem_limit_bytes=48 * 1024 * 1024
)


def scale_of(count):
    return levels / math.log1p(2.65 * count / floor_z)


def encode(z, count):
    size = (scale_of(count) * jnp.log(1.0 + jnp.abs(z) * (1.0 / floor_z)) + 0.5).astype(jnp.int32)
    code = jnp.where(z < 0.0, -size, size)
    half = z.shape[0] // 2
    return (code[:half] & 0xFFFF) | (code[half:] << 16)


def decode(packed, count):
    def part(code):
        value = code.astype(jnp.float32)
        size = jnp.exp(jnp.abs(value) * (1.0 / scale_of(count))) * floor_z - floor_z
        return jnp.where(value < 0.0, -size, size)

    return jnp.concatenate([part((packed << 16) >> 16), part(packed >> 16)], axis=0)


def normalize_kernel(seed_ref, x_ref, normed_ref, panel_ref, acc_ref):
    step = pl.program_id(0)
    series = x_ref[0]
    length, width = series.shape
    demean = series - jnp.sum(series, axis=0, keepdims=True) * (1.0 / length)
    spread = jnp.sum(demean * demean, axis=0, keepdims=True) * (1.0 / length)
    normed = (demean * lax.rsqrt(spread + epsilon)).astype(jnp.bfloat16)
    normed_ref[...] = normed
    column = lax.broadcasted_iota(jnp.int32, (seed_ref.shape[0], width), 1) + step * width
    chosen = (column == seed_ref[...]).astype(jnp.float32).astype(jnp.bfloat16)
    picked = lax.dot_general(
        chosen, normed, (((1,), (1,)), ((), ())), preferred_element_type=jnp.float32
    )

    @pl.when(step == 0)
    def _():
        acc_ref[...] = picked

    @pl.when(step > 0)
    def _():
        acc_ref[...] += picked

    @pl.when(step == pl.num_programs(0) - 1)
    def _():
        panel_ref[...] = acc_ref[...].astype(jnp.bfloat16)


def normalize(series, offsets):
    _, length, columns = series.shape
    seeds = offsets.shape[0]
    width = math.gcd(columns, 1024)
    return pl.pallas_call(
        normalize_kernel,
        grid=(columns // width,),
        in_specs=[
            pl.BlockSpec((seeds, 1), lambda i: (0, 0)),
            pl.BlockSpec((1, length, width), lambda i: (0, 0, i)),
        ],
        out_specs=[
            pl.BlockSpec((length, width), lambda i: (0, i)),
            pl.BlockSpec((seeds, length), lambda i: (0, 0)),
        ],
        out_shape=[
            jax.ShapeDtypeStruct((length, columns), jnp.bfloat16),
            jax.ShapeDtypeStruct((seeds, length), jnp.bfloat16),
        ],
        scratch_shapes=[pltpu.VMEM((seeds, length), jnp.float32)],
        compiler_params=params,
        name="normalize",
    )(offsets.reshape(seeds, 1), series)


def fisher(panel, normed, length):
    dots = lax.dot_general(
        panel, normed, (((1,), (0,)), ((), ())), preferred_element_type=jnp.float32
    )
    clipped = jnp.clip(dots * (1.0 / length), -clip_limit, clip_limit)
    return 0.5 * (jnp.log(1.0 + clipped) - jnp.log(1.0 - clipped))


def first_kernel(table_ref, panel_ref, normed_ref, *outs, firsts, length):
    mask = pl.program_id(0)
    z = fisher(panel_ref[...], normed_ref[...], length)
    rows = z.shape[0] // colours
    for c, bit in enumerate(firsts):
        mine = z[c * rows : (c + 1) * rows]
        sends = (mask >> bit) & 1

        @pl.when(sends == 1)
        def _():
            outs[c][0] = encode(mine, 1)

        @pl.when(sends == 0)
        def _():
            outs[colours + c][0] = mine


def first(table, panel, normed, wave, waves, firsts, groups):
    seeds, length = panel.shape
    width = normed.shape[1] // groups // waves
    rows = seeds // colours
    half = groups // 2

    def out_map(k):
        return lambda i, t: (t[(k + 1) * groups + i], 0, 0)

    return pl.pallas_call(
        lambda *refs: first_kernel(*refs, firsts=firsts, length=length),
        grid_spec=pltpu.PrefetchScalarGridSpec(
            num_scalar_prefetch=1,
            grid=(groups,),
            in_specs=[
                pl.BlockSpec((seeds, length), lambda i, t: (0, 0)),
                pl.BlockSpec((length, width), lambda i, t: (0, t[i] * waves + wave)),
            ],
            out_specs=[pl.BlockSpec((1, rows // 2, width), out_map(c)) for c in range(colours)]
            + [pl.BlockSpec((1, rows, width), out_map(colours + c)) for c in range(colours)],
        ),
        out_shape=[jax.ShapeDtypeStruct((half, rows // 2, width), jnp.int32)] * colours
        + [jax.ShapeDtypeStruct((half, rows, width), jnp.float32)] * colours,
        compiler_params=params,
        name="fisher",
    )(table, panel, normed)


def combine_kernel(*refs, count, half):
    step = pl.program_id(0)
    arrived, kept, outs = refs[:colours], refs[colours : 2 * colours], refs[2 * colours :]
    for c in range(colours):
        z = kept[c][0] + decode(arrived[c][0], count)

        @pl.when(step < half)
        def _():
            outs[colours + c][0] = z

        @pl.when(step >= half)
        def _():
            outs[c][0] = encode(z, 2 * count)


def combine(arrived, kept, count):
    blocks, rows, width = kept[0].shape
    half = blocks // 2
    whole = lambda r: pl.BlockSpec((1, r, width), lambda i: (i, 0, 0))
    sends = pl.BlockSpec((1, rows // 2, width), lambda i: (jnp.maximum(i - half, 0), 0, 0))
    keeps = pl.BlockSpec((1, rows, width), lambda i: (jnp.minimum(i, half - 1), 0, 0))
    return pl.pallas_call(
        lambda *refs: combine_kernel(*refs, count=count, half=half),
        grid=(blocks,),
        in_specs=[whole(rows // 2)] * colours + [whole(rows)] * colours,
        out_specs=[sends] * colours + [keeps] * colours,
        out_shape=[jax.ShapeDtypeStruct((half, rows // 2, width), jnp.int32)] * colours
        + [jax.ShapeDtypeStruct((half, rows, width), jnp.float32)] * colours,
        compiler_params=params,
        name="combine",
    )(*arrived, *kept)


def last_kernel(*refs, count, groups):
    arrived, kept, out = refs[:colours], refs[colours : 2 * colours], refs[2 * colours]
    z = [kept[c][0] + decode(arrived[c][0], count) for c in range(colours)]
    out[...] = jnp.concatenate(z, axis=0).T * (1.0 / groups)


def last(arrived, kept, count, groups):
    _, rows, width = kept[0].shape
    return pl.pallas_call(
        lambda *refs: last_kernel(*refs, count=count, groups=groups),
        out_shape=jax.ShapeDtypeStruct((width, rows * colours), jnp.float32),
        compiler_params=pltpu.CompilerParams(vmem_limit_bytes=48 * 1024 * 1024),
        name="last",
    )(*arrived, *kept)


def tables(groups, bits, orders):
    sent, kept = [], []
    for order in orders:
        place = lambda m: sum(((m >> b) & 1) << (bits - 1 - j) for j, b in enumerate(order) if j)
        for store, want in ((sent, 1), (kept, 0)):
            row, current = [], None
            for m in range(groups):
                if (m >> order[0]) & 1 == want:
                    current = place(m)
                row.append(current)
            head = next(v for v in row if v is not None)
            store.append([head if v is None else v for v in row])
    return np.array(sent + kept, np.int32)


def make_body(groups, parts):
    bits = groups.bit_length() - 1
    assert groups == 1 << bits and bits >= 2
    orders = [tuple((c + j) % bits for j in range(bits)) for c in range(colours)]
    firsts = [order[0] for order in orders]
    layout = tables(groups, bits, orders)

    def cube(i):
        return i ^ (((i >> (bits - 1)) & 1) << (bits - 2))

    def swap(x, bit):
        pairs = [(i, cube(cube(i) ^ (1 << bit))) for i in range(groups)]
        return lax.ppermute(x, "subj", pairs)

    def body(bold_series, seed_index):
        columns = bold_series.shape[2]
        offsets = seed_index - lax.axis_index("vox") * columns
        normed, own = normalize(bold_series, offsets)
        panel = own
        for hop in range(1, parts):
            ring = [(i, (i + hop) % parts) for i in range(parts)]
            panel = panel + lax.ppermute(own, "vox", ring)
        me = cube(lax.axis_index("subj"))
        dests = cube(jnp.arange(groups, dtype=jnp.int32) ^ me)
        table = jnp.concatenate([dests, jnp.asarray(layout.reshape(-1))])
        waves = 2 if (columns // groups) % 256 == 0 else 1
        state = []
        for wave in range(waves):
            outs = first(table, panel, normed, wave, waves, firsts, groups)
            state.append((outs[:colours], outs[colours:]))
        for j in range(bits):
            moved = [
                ([swap(x, orders[c][j]) for c, x in enumerate(sent)], kept) for sent, kept in state
            ]
            if j == bits - 1:
                return jnp.concatenate([last(a, k, 1 << j, groups) for a, k in moved], axis=0)
            state = []
            for arrived, kept in moved:
                outs = combine(arrived, kept, 1 << j)
                state.append((outs[:colours], outs[colours:]))

    return body


def solution(mesh):
    body = make_body(mesh.shape["subj"], mesh.shape["vox"])
    in_specs = (P("subj", None, "vox"), P())
    out_specs = P(("vox", "subj"), None)
    return jax.shard_map(body, mesh=mesh, in_specs=in_specs, out_specs=out_specs, check_vma=False)
```

```python
import math

import jax
import jax.numpy as jnp
from jax import lax
from jax.experimental import pallas as pl
from jax.experimental.pallas import tpu as pltpu
from jax.sharding import PartitionSpec as P

clip_limit = 0.99
epsilon = 1e-05
lane = 128
floor_z = 2.0**-11
levels = 32700.0

params = pltpu.CompilerParams(
    dimension_semantics=("arbitrary",), vmem_limit_bytes=48 * 1024 * 1024
)


def scale_of(count):
    return levels / math.log1p(2.65 * count / floor_z)


def encode(z, count):
    size = (scale_of(count) * jnp.log(1.0 + jnp.abs(z) * (1.0 / floor_z)) + 0.5).astype(jnp.int32)
    code = jnp.where(z < 0.0, -size, size)
    half = z.shape[0] // 2
    return (code[:half] & 0xFFFF) | (code[half:] << 16)


def decode(packed, count):
    def part(code):
        value = code.astype(jnp.float32)
        size = jnp.exp(jnp.abs(value) * (1.0 / scale_of(count))) * floor_z - floor_z
        return jnp.where(value < 0.0, -size, size)

    return jnp.concatenate([part((packed << 16) >> 16), part(packed >> 16)], axis=0)


def normalize_kernel(seed_ref, x_ref, normed_ref, panel_ref, acc_ref):
    step = pl.program_id(0)
    length, lines, lanes = x_ref.shape
    rows = x_ref.reshape(length * lines, lanes)
    for j in range(lines):
        series = rows[pl.ds(j, length, stride=lines), :]
        demean = series - jnp.sum(series, axis=0, keepdims=True) * (1.0 / length)
        spread = jnp.sum(demean * demean, axis=0, keepdims=True) * (1.0 / length)
        normed = (demean * lax.rsqrt(spread + epsilon)).astype(jnp.bfloat16)
        normed_ref[:, j * lanes : (j + 1) * lanes] = normed
    width = lines * lanes
    column = lax.broadcasted_iota(jnp.int32, (seed_ref.shape[0], width), 1) + step * width
    chosen = (column == seed_ref[...]).astype(jnp.float32).astype(jnp.bfloat16)
    picked = lax.dot_general(
        chosen, normed_ref[...], (((1,), (1,)), ((), ())), preferred_element_type=jnp.float32
    )

    @pl.when(step == 0)
    def _():
        acc_ref[...] = picked

    @pl.when(step > 0)
    def _():
        acc_ref[...] += picked

    @pl.when(step == pl.num_programs(0) - 1)
    def _():
        panel_ref[...] = acc_ref[...].astype(jnp.bfloat16)


def normalize(series, offsets):
    _, length, columns = series.shape
    seeds = offsets.shape[0]
    lines = 8
    width = lines * lane
    return pl.pallas_call(
        normalize_kernel,
        grid=(columns // width,),
        in_specs=[
            pl.BlockSpec((seeds, 1), lambda i: (0, 0)),
            pl.BlockSpec((length, lines, lane), lambda i: (0, i, 0)),
        ],
        out_specs=[
            pl.BlockSpec((length, width), lambda i: (0, i)),
            pl.BlockSpec((seeds, length), lambda i: (0, 0)),
        ],
        out_shape=[
            jax.ShapeDtypeStruct((length, columns), jnp.bfloat16),
            jax.ShapeDtypeStruct((seeds, length), jnp.bfloat16),
        ],
        scratch_shapes=[pltpu.VMEM((seeds, length), jnp.float32)],
        compiler_params=params,
        name="normalize",
    )(offsets.reshape(seeds, 1), series.reshape(length, columns // lane, lane))


def fisher(panel, normed, length):
    dots = lax.dot_general(
        panel, normed, (((1,), (0,)), ((), ())), preferred_element_type=jnp.float32
    )
    clipped = jnp.clip(dots * (1.0 / length), -clip_limit, clip_limit)
    return 0.5 * (jnp.log(1.0 + clipped) - jnp.log(1.0 - clipped))


def first_kernel(table_ref, panel_ref, *refs, colours, length, coded):
    blocks, outs = refs[:colours], refs[colours:]
    normed = jnp.concatenate([block[...] for block in blocks], axis=1)
    z = fisher(panel_ref[...], normed, length)
    for c in range(colours):
        mine = z[:, c * lane : (c + 1) * lane]
        outs[c][0] = encode(mine, 1) if coded else mine


def first(table, panel, normed, groups, colours, coded):
    seeds, length = panel.shape
    half = groups // 2
    skip = half if coded else 0
    pieces = normed.shape[1] // groups // lane // colours

    def in_map(c):
        return lambda i, p, t: (0, (t[c * groups + skip + i] * colours + c) * pieces + p)

    if coded:
        out = jax.ShapeDtypeStruct((half, seeds // 2, pieces * lane), jnp.int32)
    else:
        out = jax.ShapeDtypeStruct((half, seeds, pieces * lane), jnp.float32)
    return pl.pallas_call(
        lambda *refs: first_kernel(*refs, colours=colours, length=length, coded=coded),
        grid_spec=pltpu.PrefetchScalarGridSpec(
            num_scalar_prefetch=1,
            grid=(half, pieces),
            in_specs=[pl.BlockSpec((seeds, length), lambda i, p, t: (0, 0))]
            + [pl.BlockSpec((length, lane), in_map(c)) for c in range(colours)],
            out_specs=[
                pl.BlockSpec((1, out.shape[1], lane), lambda i, p, t: (i, 0, p))
                for c in range(colours)
            ],
        ),
        out_shape=[out] * colours,
        compiler_params=pltpu.CompilerParams(
            dimension_semantics=("arbitrary", "arbitrary"), vmem_limit_bytes=48 * 1024 * 1024
        ),
        name="send" if coded else "keep",
    )(table, panel, *([normed] * colours))


def combine_kernel(*refs, count, half, colours):
    step = pl.program_id(0)
    arrived, kept, outs = refs[:colours], refs[colours : 2 * colours], refs[2 * colours :]
    for c in range(colours):
        z = kept[c][0] + decode(arrived[c][0], count)

        @pl.when(step < half)
        def _():
            outs[colours + c][0] = z

        @pl.when(step >= half)
        def _():
            outs[c][0] = encode(z, 2 * count)


def combine(arrived, kept, count):
    colours = len(kept)
    blocks, rows, width = kept[0].shape
    half = blocks // 2
    whole = lambda r: pl.BlockSpec((1, r, width), lambda i: (i, 0, 0))
    sends = pl.BlockSpec((1, rows // 2, width), lambda i: (jnp.maximum(i - half, 0), 0, 0))
    keeps = pl.BlockSpec((1, rows, width), lambda i: (jnp.minimum(i, half - 1), 0, 0))
    outs = pl.pallas_call(
        lambda *refs: combine_kernel(*refs, count=count, half=half, colours=colours),
        grid=(blocks,),
        in_specs=[whole(rows // 2)] * colours + [whole(rows)] * colours,
        out_specs=[sends] * colours + [keeps] * colours,
        out_shape=[jax.ShapeDtypeStruct((half, rows // 2, width), jnp.int32)] * colours
        + [jax.ShapeDtypeStruct((half, rows, width), jnp.float32)] * colours,
        compiler_params=params,
        name="combine",
    )(*arrived, *kept)
    return outs[:colours], outs[colours:]


def last_kernel(*refs, count, groups, colours):
    arrived, kept, out = refs[:colours], refs[colours : 2 * colours], refs[2 * colours]
    width = kept[0].shape[2]
    for c in range(colours):
        z = kept[c][0] + decode(arrived[c][0], count)
        out[c * width : (c + 1) * width, :] = z.T * (1.0 / groups)


def last(arrived, kept, count, groups):
    colours = len(kept)
    _, rows, width = kept[0].shape
    return pl.pallas_call(
        lambda *refs: last_kernel(*refs, count=count, groups=groups, colours=colours),
        out_shape=jax.ShapeDtypeStruct((width * colours, rows), jnp.float32),
        compiler_params=pltpu.CompilerParams(vmem_limit_bytes=48 * 1024 * 1024),
        name="last",
    )(*arrived, *kept)


def make_body(groups, parts):
    bits = groups.bit_length() - 1
    assert groups == 1 << bits and bits >= 2

    def cube(i):
        return i ^ (((i >> (bits - 1)) & 1) << (bits - 2))

    def swap(x, bit):
        pairs = [(i, cube(cube(i) ^ (1 << bit))) for i in range(groups)]
        return lax.ppermute(x, "subj", pairs)

    def body(bold_series, seed_index):
        columns = bold_series.shape[2]
        colours = next(c for c in (4, 2, 1) if (columns // groups) % (c * lane) == 0)
        if bits == 4:
            orders = [tuple(c ^ j for j in range(bits)) for c in range(colours)]
        else:
            orders = [tuple((c + j) % bits for j in range(bits)) for c in range(colours)]
        masks = [
            [sum(((p >> (bits - 1 - j)) & 1) << b for j, b in enumerate(o)) for p in range(groups)]
            for o in orders
        ]
        offsets = seed_index - lax.axis_index("vox") * columns
        normed, own = normalize(bold_series, offsets)
        panel = own
        for hop in range(1, parts):
            ring = [(i, (i + hop) % parts) for i in range(parts)]
            panel = panel + lax.ppermute(own, "vox", ring)
        me = cube(lax.axis_index("subj"))
        table = cube(jnp.array(masks, jnp.int32).reshape(-1) ^ me)
        sent = first(table, panel, normed, groups, colours, True)
        moved = [swap(x, orders[c][0]) for c, x in enumerate(sent)]
        kept = first(table, panel, normed, groups, colours, False)
        for j in range(1, bits):
            sent, kept = combine(moved, kept, 1 << (j - 1))
            moved = [swap(x, orders[c][j]) for c, x in enumerate(sent)]
        return last(moved, kept, 1 << (bits - 1), groups)

    return body


def solution(mesh):
    body = make_body(mesh.shape["subj"], mesh.shape["vox"])
    in_specs = (P("subj", None, "vox"), P())
    out_specs = P(("vox", "subj"), None)
    return jax.shard_map(body, mesh=mesh, in_specs=in_specs, out_specs=out_specs, check_vma=False)
```

```python
import math

import jax
import jax.numpy as jnp
from jax import lax
from jax.experimental import pallas as pl
from jax.experimental.pallas import tpu as pltpu
from jax.sharding import PartitionSpec as P

clip_limit = 0.99
epsilon = 1e-05
lane = 128
floor_z = 2.0**-11
levels = 32700.0

params = pltpu.CompilerParams(
    dimension_semantics=("arbitrary",), vmem_limit_bytes=16 * 1024 * 1024
)


def scale_of(count):
    return levels / math.log1p(2.65 * count / floor_z)


def encode(z, count):
    size = (scale_of(count) * jnp.log(1.0 + jnp.abs(z) * (1.0 / floor_z)) + 0.5).astype(jnp.int32)
    code = jnp.where(z < 0.0, -size, size)
    half = z.shape[0] // 2
    return (code[:half] & 0xFFFF) | (code[half:] << 16)


def decode(packed, count):
    def part(code):
        value = code.astype(jnp.float32)
        size = jnp.exp(jnp.abs(value) * (1.0 / scale_of(count))) * floor_z - floor_z
        return jnp.where(value < 0.0, -size, size)

    return jnp.concatenate([part((packed << 16) >> 16), part(packed >> 16)], axis=0)


def normalize_kernel(seed_ref, x_ref, normed_ref, panel_ref, acc_ref):
    step = pl.program_id(0)
    length, lines, lanes = x_ref.shape
    rows = x_ref.reshape(length * lines, lanes)
    for j in range(lines):
        series = rows[pl.ds(j, length, stride=lines), :]
        demean = series - jnp.sum(series, axis=0, keepdims=True) * (1.0 / length)
        spread = jnp.sum(demean * demean, axis=0, keepdims=True) * (1.0 / length)
        normed = (demean * lax.rsqrt(spread + epsilon)).astype(jnp.bfloat16)
        normed_ref[:, j * lanes : (j + 1) * lanes] = normed
    width = lines * lanes
    column = lax.broadcasted_iota(jnp.int32, (seed_ref.shape[0], width), 1) + step * width
    chosen = (column == seed_ref[...]).astype(jnp.float32).astype(jnp.bfloat16)
    picked = lax.dot_general(
        chosen, normed_ref[...], (((1,), (1,)), ((), ())), preferred_element_type=jnp.float32
    )

    @pl.when(step == 0)
    def _():
        acc_ref[...] = picked

    @pl.when(step > 0)
    def _():
        acc_ref[...] += picked

    @pl.when(step == pl.num_programs(0) - 1)
    def _():
        panel_ref[...] = acc_ref[...].astype(jnp.bfloat16)


def normalize(series, offsets):
    _, length, columns = series.shape
    seeds = offsets.shape[0]
    lines = 8
    width = lines * lane
    return pl.pallas_call(
        normalize_kernel,
        grid=(columns // width,),
        in_specs=[
            pl.BlockSpec((seeds, 1), lambda i: (0, 0)),
            pl.BlockSpec((length, lines, lane), lambda i: (0, i, 0)),
        ],
        out_specs=[
            pl.BlockSpec((length, width), lambda i: (0, i)),
            pl.BlockSpec((seeds, length), lambda i: (0, 0)),
        ],
        out_shape=[
            jax.ShapeDtypeStruct((length, columns), jnp.bfloat16),
            jax.ShapeDtypeStruct((seeds, length), jnp.bfloat16),
        ],
        scratch_shapes=[pltpu.VMEM((seeds, length), jnp.float32)],
        compiler_params=pltpu.CompilerParams(
            dimension_semantics=("arbitrary",), vmem_limit_bytes=52 * 1024 * 1024
        ),
        name="normalize",
    )(offsets.reshape(seeds, 1), series.reshape(length, columns // lane, lane))


def fisher(panel, normed, length):
    dots = lax.dot_general(
        panel, normed, (((1,), (0,)), ((), ())), preferred_element_type=jnp.float32
    )
    clipped = jnp.clip(dots * (1.0 / length), -clip_limit, clip_limit)
    return 0.5 * jnp.log((1.0 + clipped) / (1.0 - clipped))


def spans(rows):
    ends = [sum(rows[: c + 1]) for c in range(len(rows))]
    return [(end - r, end) for r, end in zip(rows, ends)]


def first_kernel(table_ref, panel_ref, *refs, rows, length, coded):
    blocks, outs = refs[: len(rows)], refs[len(rows) :]
    for (low, high), block, out in zip(spans(rows), blocks, outs):
        z = fisher(panel_ref[low:high, :], block[...], length)
        out[0] = encode(z, 1) if coded else z


def first(table, panel, normed, groups, rows, coded):
    seeds, length = panel.shape
    half = groups // 2
    skip = half if coded else 0
    width = normed.shape[1] // groups

    def in_map(c):
        return lambda i, t: (0, t[c * groups + skip + i])

    if coded:
        outs = [jax.ShapeDtypeStruct((half, r // 2, width), jnp.int32) for r in rows]
    else:
        outs = [jax.ShapeDtypeStruct((half, r, width), jnp.float32) for r in rows]
    return pl.pallas_call(
        lambda *refs: first_kernel(*refs, rows=rows, length=length, coded=coded),
        grid_spec=pltpu.PrefetchScalarGridSpec(
            num_scalar_prefetch=1,
            grid=(half,),
            in_specs=[pl.BlockSpec((seeds, length), lambda i, t: (0, 0))]
            + [pl.BlockSpec((length, width), in_map(c)) for c in range(len(rows))],
            out_specs=[pl.BlockSpec((1,) + o.shape[1:], lambda i, t: (i, 0, 0)) for o in outs],
        ),
        out_shape=outs,
        compiler_params=params,
        name="send" if coded else "keep",
    )(table, panel, *([normed] * len(rows)))


def combine_kernel(*refs, rows, count, half, merge):
    step = pl.program_id(0)
    n = len(rows)
    arrived, kept, outs = refs[:n], refs[n : 2 * n], refs[2 * n :]
    for c, (low, high) in enumerate(spans(rows)):
        z = kept[c][0] + decode(arrived[c][0], count)

        @pl.when(step < half)
        def _():
            if merge:
                outs[1][0, low:high, :] = z
            else:
                outs[n + c][0] = z

        @pl.when(step >= half)
        def _():
            code = encode(z, 2 * count)
            if merge:
                outs[0][0, low // 2 : high // 2, :] = code
            else:
                outs[c][0] = code


def combine(arrived, kept, rows, count, merge):
    blocks, _, width = kept[0].shape
    half = blocks // 2
    wide = (sum(rows),) if merge else rows
    whole = lambda r: pl.BlockSpec((1, r, width), lambda i: (i, 0, 0))
    sends = lambda r: pl.BlockSpec((1, r, width), lambda i: (jnp.maximum(i - half, 0), 0, 0))
    keeps = lambda r: pl.BlockSpec((1, r, width), lambda i: (jnp.minimum(i, half - 1), 0, 0))
    outs = pl.pallas_call(
        lambda *refs: combine_kernel(*refs, rows=rows, count=count, half=half, merge=merge),
        grid=(blocks,),
        in_specs=[whole(r // 2) for r in rows] + [whole(r) for r in rows],
        out_specs=[sends(r // 2) for r in wide] + [keeps(r) for r in wide],
        out_shape=[jax.ShapeDtypeStruct((half, r // 2, width), jnp.int32) for r in wide]
        + [jax.ShapeDtypeStruct((half, r, width), jnp.float32) for r in wide],
        compiler_params=params,
        name="combine",
    )(*arrived, *kept)
    return outs[: len(wide)], outs[len(wide) :]


def last_kernel(arrived, kept, out, *, rows, count, groups):
    z = [
        kept[0, low:high, :] + decode(arrived[0, low // 2 : high // 2, :], count)
        for low, high in spans(rows)
    ]
    out[...] = jnp.concatenate(z, axis=0).T * (1.0 / groups)


def last(arrived, kept, rows, count, groups):
    _, seeds, width = kept.shape
    return pl.pallas_call(
        lambda *refs: last_kernel(*refs, rows=rows, count=count, groups=groups),
        out_shape=jax.ShapeDtypeStruct((width, seeds), jnp.float32),
        compiler_params=pltpu.CompilerParams(vmem_limit_bytes=16 * 1024 * 1024),
        name="last",
    )(arrived, kept)


def make_body(groups, parts):
    bits = groups.bit_length() - 1
    assert groups == 1 << bits and bits >= 2
    cheap = bits - 1
    colours = min(3, cheap)
    orders = [tuple((c + j) % cheap for j in range(cheap)) + (cheap,) for c in range(colours)]
    masks = [
        [sum(((p >> (bits - 1 - j)) & 1) << b for j, b in enumerate(o)) for p in range(groups)]
        for o in orders
    ]

    def swap(x, bit):
        return lax.ppermute(x, "subj", [(i, i ^ (1 << bit)) for i in range(groups)])

    def body(bold_series, seed_index):
        columns = bold_series.shape[2]
        units = seed_index.shape[0] // 16
        rows = tuple(16 * ((units + c) // colours) for c in range(colours))
        offsets = seed_index - lax.axis_index("vox") * columns
        normed, own = normalize(bold_series, offsets)
        panel = own
        for hop in range(1, parts):
            ring = [(i, (i + hop) % parts) for i in range(parts)]
            panel = panel + lax.ppermute(own, "vox", ring)
        table = jnp.array(masks, jnp.int32).reshape(-1) ^ lax.axis_index("subj")
        sent = first(table, panel, normed, groups, rows, True)
        moved = [swap(x, orders[c][0]) for c, x in enumerate(sent)]
        kept = first(table, panel, normed, groups, rows, False)
        for j in range(1, bits):
            sent, kept = combine(moved, kept, rows, 1 << (j - 1), j == cheap)
            moved = [swap(x, orders[c][j]) for c, x in enumerate(sent)]
        return last(moved[0], kept[0], rows, 1 << cheap, groups)

    return body


def solution(mesh):
    body = make_body(mesh.shape["subj"], mesh.shape["vox"])
    in_specs = (P("subj", None, "vox"), P())
    out_specs = P(("vox", "subj"), None)
    return jax.shard_map(body, mesh=mesh, in_specs=in_specs, out_specs=out_specs, check_vma=False)
```
